256 devices in a mesh: group: 4 (over x), dp: 16 (over z_lo, y, core), mp: 4 (over z_hi).
Axes of the slice: x: 4, y: 4, z: 8 (z_hi: 4, z_lo: 2; z = z_hi * 2 + z_lo), core: 2. Of those that a mesh axis runs over, the one named last changes fastest.
Arguments:
- block_input: bfloat16 [768, 8192], P(None, 'dp'), may hold values from -6 to 6
- parent_gate_up: bfloat16 [2, 8192, 14336], P(None, 'dp', ('group', 'mp')), may hold values from -0.0625 to 0.0625
- parent_down: bfloat16 [14336, 8192], P(('group', 'mp'), 'dp'), may hold values from -0.046875 to 0.046875
- variant_gate_up: bfloat16 [4, 2, 8192, 3584], P('group', None, 'dp', 'mp'), may hold values from -0.0625 to 0.0625
- variant_down: bfloat16 [4, 3584, 8192], P('group', 'mp', 'dp'), may hold values from -0.09375 to 0.09375
- widths: int32 [4], P('group'), may hold values from 896 to 3584, as said below
Outputs:
- grad_gate_up: float32 [4, 2, 8192, 3584], P('group', None, 'dp', 'mp')
- grad_down: float32 [4, 3584, 8192], P('group', 'mp', 'dp')
The draws below stay inside these ranges and needn't reach their ends.
Inputs may be any that keep to these rules, and one draw needn't show every extreme that they name: Variant v uses its hidden units 0 to widths[v] - 1; one variant uses all 3584 of them and another exactly a quarter of 3584.
All inputs are finite; a program needn't handle non-finite values.
Results may differ from the reference program's by a relative error of at most 0.008.
Values may be sent and summed in bfloat16 or wider, within the bound.
No kernel may reach another device: no remote copies, remote signals or barrier semaphores. Data moves between devices by JAX's collectives and lax.ppermute only.
A program may use at most 64 MiB of HBM per device.

```python
import math
import jax
import jax.numpy as jnp

D = 8192
FF = 14336
FV = 3584
TOKENS = 768
VARIANTS = 4


def draw_widths(key, part):
    base_widths = jax.random.randint(key, (VARIANTS,), FV // 4, FV + 1)
    widest = jax.random.randint(jax.random.fold_in(key, 11), (), 0, VARIANTS)
    offset = jax.random.randint(jax.random.fold_in(key, 13), (), 1, VARIANTS)
    narrowest = (widest + offset) % VARIANTS
    slot_index = jnp.arange(VARIANTS)
    chosen = jnp.where(slot_index == widest, FV, base_widths)
    chosen = jnp.where(slot_index == narrowest, FV // 4, chosen)
    return chosen.astype(jnp.int32)


def strengthened(entries, rng, source, target, parts, factor):
    def block_of(dim):
        return (jnp.arange(entries.shape[dim]) // (entries.shape[dim] // parts)).reshape((-1,) + (1,) * (entries.ndim - 1 - dim))

    near = jax.random.permutation(rng, parts)[block_of(target)]
    other_side = (block_of(target) + parts // 2) % parts
    return jnp.where((block_of(source) == near) | (block_of(source) == other_side), factor * entries, entries)


def shard_levels(rng, dims, shards, low, high):
    level, own = 1.0, jax.random.fold_in(rng, 6)
    for axis_at, blocks in shards:
        draws = jnp.exp(jax.random.uniform(jax.random.fold_in(own, axis_at), (blocks,), jnp.float32, low / len(shards), high / len(shards)))
        level = level * jnp.repeat(draws, dims[axis_at] // blocks).reshape([-1 if axis == axis_at else 1 for axis in range(len(dims))])
    return level


def gaussian(key, shape, deviation, limit, split=(), held_as=jnp.bfloat16):
    result = deviation * jax.random.normal(key, shape, jnp.float32)
    if split:
        result = result * shard_levels(key, shape, split, -0.22, 0.18)
    return jnp.clip(result, -limit, limit).astype(held_as)


def noise_with(rng, extent, width, limit, pieces, heavy, held_as=jnp.bfloat16):
    drawn = width * jax.random.normal(rng, extent, jnp.float32)
    if pieces:
        drawn = drawn * shard_levels(rng, extent, pieces, -0.22, 0.18)
    return jnp.clip(strengthened(drawn, jax.random.fold_in(rng, 3), *heavy), -limit, limit).astype(held_as)


def setup_inputs(seed: int = 0) -> dict:
    key_list = jax.random.split(jax.random.key(seed), 7)
    return {
        "block_input": noise_with(key_list[0], (TOKENS, D), 1.0, 6.0, ((1, 16),), (1, 0, 16, 2.0)),
        "parent_gate_up": gaussian(key_list[1], (2, D, FF), D ** -0.5, 0.0625, ((1, 16), (2, 16))),
        "parent_down": gaussian(key_list[2], (FF, D), FF ** -0.5, 0.046875, ((0, 16), (1, 16))),
        "variant_gate_up": gaussian(key_list[3], (VARIANTS, 2, D, FV), D ** -0.5, 0.0625, ((0, 4), (2, 16), (3, 4))),
        "variant_down": gaussian(key_list[4], (VARIANTS, FV, D), FV ** -0.5, 0.09375, ((0, 4), (1, 4), (2, 16))),
        "widths": draw_widths(jax.random.fold_in(key_list[6], 71), 0),
    }


def gated_values(pre_act, unit_mask):
    gate_value = pre_act[:, 0].astype(jnp.float32)
    up_value = pre_act[:, 1].astype(jnp.float32)
    sigmoid_gate = jax.nn.sigmoid(gate_value)
    return (gate_value * sigmoid_gate * up_value * unit_mask).astype(jnp.bfloat16)

def pre_gradient(pre_act, unit_mask, hidden_grad):
    gate_value = pre_act[:, 0].astype(jnp.float32)
    up_value = pre_act[:, 1].astype(jnp.float32)
    sigmoid_gate = jax.nn.sigmoid(gate_value)
    masked_grad = hidden_grad * unit_mask
    grad_gate = masked_grad * up_value * sigmoid_gate * (1.0 + gate_value * (1.0 - sigmoid_gate))
    grad_up = masked_grad * gate_value * sigmoid_gate
    return jnp.stack([grad_gate, grad_up], axis=1).astype(jnp.bfloat16)

def reference(block_input, parent_gate_up, parent_down, variant_gate_up, variant_down, widths):
    loss_scale = 1.0 / math.sqrt(TOKENS)
    parent_pre = jnp.stack([jnp.dot(block_input, parent_gate_up[member], preferred_element_type=jnp.float32) for member in range(2)], axis=1).astype(jnp.bfloat16)
    parent_hidden = gated_values(parent_pre, 1.0)
    teacher = jnp.dot(parent_hidden, parent_down, preferred_element_type=jnp.float32)
    unit_index = jnp.arange(FV, dtype=jnp.int32)
    grads_gate_up = []
    grads_down = []
    for variant in range(VARIANTS):
        variant_pre = jnp.stack([jnp.dot(block_input, variant_gate_up[variant, member], preferred_element_type=jnp.float32) for member in range(2)], axis=1).astype(jnp.bfloat16)
        unit_mask = (unit_index < widths[variant]).astype(jnp.float32)
        variant_hidden = gated_values(variant_pre, unit_mask)
        student = jnp.dot(variant_hidden, variant_down[variant], preferred_element_type=jnp.float32)
        output_grad = ((student - teacher) * loss_scale).astype(jnp.bfloat16)
        grads_down.append(jnp.dot(variant_hidden.T, output_grad, preferred_element_type=jnp.float32))
        hidden_grad = jnp.dot(output_grad, variant_down[variant].T, preferred_element_type=jnp.float32)
        grad_pre = pre_gradient(variant_pre, unit_mask, hidden_grad)
        grads_gate_up.append(jnp.stack([jnp.dot(block_input.T, grad_pre[:, member], preferred_element_type=jnp.float32) for member in range(2)], axis=0))
    return (jnp.stack(grads_gate_up, axis=0), jnp.stack(grads_down, axis=0))
```

```python
import math

import jax
import jax.numpy as jnp
from jax import lax
from jax.experimental import pallas as pl
from jax.experimental.pallas import tpu as pltpu
from jax.sharding import Mesh
from jax.sharding import PartitionSpec as P

BF, F32 = jnp.bfloat16, jnp.float32
DIMS = {"c": ("core", 1), "a": ("y", 1), "b": ("y", 3), "z": ("zl", 1)}
ORDERS = ("abz", "bza", "zab")


def swap(value, axis, mask):
    size = {"core": 2, "y": 4, "zl": 2, "group": 4, "mp": 4}[axis]
    return lax.ppermute(value, axis, [(i, i ^ mask) for i in range(size)])


def pick(value, axis, index):
    return lax.index_in_dim(value, index, axis, keepdims=False)


def dim_axis(left, dim):
    return 2 + left.index(dim)


def relative_rows(block_input):
    rows, width = block_input.shape

    def kernel(x_ref, o_ref):
        y, z, core = lax.axis_index("y"), lax.axis_index("zl"), lax.axis_index("core")
        owner = ((y ^ (y >> 1)) & 1) * 4 + (y >> 1) * 2 + z
        for block in range(rows // 8):
            half, inner = divmod(block, rows // 16)
            stream, at = divmod(inner, 8)
            o_ref[block] = x_ref[(half ^ core) * (rows // 16) + stream * 8 + (at ^ owner)]

    out = pl.pallas_call(
        kernel,
        out_shape=jax.ShapeDtypeStruct((rows // 8, 8, width), BF),
        in_specs=[pl.BlockSpec(memory_space=pltpu.VMEM)],
        out_specs=pl.BlockSpec(memory_space=pltpu.VMEM),
        cost_estimate=pl.CostEstimate(flops=1000000, bytes_accessed=4 * rows * width, transcendentals=0),
    )(block_input.reshape(rows // 8, 8, width))
    return out.reshape(rows, width)


def gate_up_gradient(x_t, gate_all, up_all, unit_mask, hidden_grad):
    width, rows = x_t.shape
    units, n = gate_all.shape[1], 128

    def kernel(x_ref, g_ref, u_ref, m_ref, h_ref, o_ref):
        grads = pre_gradient(g_ref[...], u_ref[...], m_ref[...], h_ref[...])
        out = jnp.dot(x_ref[...], jnp.concatenate(grads, axis=1), preferred_element_type=F32)
        o_ref[0] = out[:, :n]
        o_ref[1] = out[:, n:]

    column = pl.BlockSpec((rows, n), lambda i: (0, i))
    return pl.pallas_call(
        kernel,
        grid=(units // n,),
        in_specs=[
            pl.BlockSpec((width, rows), lambda i: (0, 0)),
            column,
            column,
            pl.BlockSpec((1, n), lambda i: (0, i)),
            column,
        ],
        out_specs=pl.BlockSpec((2, width, n), lambda i: (0, 0, i)),
        out_shape=jax.ShapeDtypeStruct((2, width, units), F32),
        compiler_params=pltpu.CompilerParams(dimension_semantics=("arbitrary",)),
        cost_estimate=pl.CostEstimate(
            flops=4 * rows * width * units, bytes_accessed=8 * width * units, transcendentals=rows * units
        ),
    )(x_t, gate_all, up_all, unit_mask.reshape(1, units), hidden_grad)


def owner_view(value):
    return value.reshape(6, 2, 2, 2, value.shape[0] // 48, value.shape[1])


def scatter_stream(kinds, order):
    left = "abz"
    axis = 1 + left.index(order[0])
    send = jnp.stack([(pick(k, axis, 1).astype(F32) + pick(r, axis, 1).astype(F32)).astype(BF) for k, r in kinds])
    keep = jnp.stack([pick(k, axis, 0).astype(F32) + pick(r, axis, 0).astype(F32) for k, r in kinds])
    for step, dim in enumerate(order):
        got = swap(send, *DIMS[dim])
        left = left.replace(dim, "")
        if step == 2:
            return keep + got.astype(F32)
        axis = dim_axis(left, order[step + 1])
        send = pick(keep, axis, 1) + pick(got, axis, 1).astype(F32)
        if step == 0:
            send = send.astype(BF)
        keep = pick(keep, axis, 0) + pick(got, axis, 0).astype(F32)


def gather_stream(value, order):
    left = ""
    for dim in reversed(order):
        got = swap(value, *DIMS[dim])
        left = "".join(sorted(left + dim))
        value = jnp.stack([value, got], axis=dim_axis(left, dim))
    return value


def gated(gate_value, up_value, unit_mask):
    gate_value, up_value = gate_value.astype(F32), up_value.astype(F32)
    return (gate_value * jax.nn.sigmoid(gate_value) * up_value * unit_mask).astype(BF)


def pre_gradient(gate_value, up_value, unit_mask, hidden_grad):
    gate_value, up_value = gate_value.astype(F32), up_value.astype(F32)
    s = jax.nn.sigmoid(gate_value)
    masked = hidden_grad.astype(F32) * unit_mask
    grad_gate = masked * up_value * s * (1.0 + gate_value * (1.0 - s))
    grad_up = masked * gate_value * s
    return grad_gate.astype(BF), grad_up.astype(BF)


def both_halves(x_rows, weight):
    half = x_rows.shape[0] // 2
    there = jnp.dot(x_rows[half:], weight, preferred_element_type=F32).astype(BF)
    here = jnp.dot(x_rows[:half], weight, preferred_element_type=F32)
    return there, here


def whole_rows(streams, kind):
    parts = [s[kind] for s in streams]
    value = jnp.concatenate(parts, axis=0)
    return value.reshape(-1, value.shape[-1])


def teacher_rows(part):
    g, m = lax.axis_index("group"), lax.axis_index("mp")

    def sub(i):
        return lax.dynamic_index_in_dim(part, i, 1, keepdims=False)

    total = sub(g).astype(F32)
    for mask in (2, 1, 3):
        total = total + swap(sub(g ^ mask), "group", mask).astype(F32)
    sent = total.astype(BF)
    own = lax.dynamic_index_in_dim(total, m, 0, keepdims=False)
    for mask in (2, 1, 3):
        own = own + swap(lax.dynamic_index_in_dim(sent, m ^ mask, 0, keepdims=False), "mp", mask).astype(F32)
    mine = own.astype(BF)
    relative = [mine, swap(mine, "group", 1), swap(mine, "group", 2), swap(mine, "group", 3)]
    return ordered(relative, g)


def ordered(relative, index):
    stacked = jnp.stack(relative)
    return jnp.stack([lax.dynamic_index_in_dim(stacked, index ^ i, 0, keepdims=False) for i in range(4)])


def student_quarter(part, first, second):
    m = lax.axis_index("mp")

    def quarter(i):
        return lax.dynamic_index_in_dim(part, i, 0, keepdims=False)

    got = swap(jnp.stack([quarter(m ^ first), quarter(m ^ first ^ second)]).astype(BF), "mp", first).astype(F32)
    send = quarter(m ^ second).astype(F32) + got[1]
    keep = quarter(m).astype(F32) + got[0]
    return keep + swap(send.astype(BF), "mp", second).astype(F32)


def gather_quarters(own, first, second):
    m = lax.axis_index("mp")
    got = swap(own, "mp", first)
    far = swap(jnp.stack([own, got]), "mp", second)
    relative = [None] * 4
    relative[0], relative[first], relative[second], relative[first ^ second] = own, got, far[0], far[1]
    return ordered(relative, m)


def body(block_input, parent_gate_up, parent_down, variant_gate_up, variant_down, widths):
    local_gate_up = variant_gate_up[0]
    local_down = variant_down[0]
    local_units = local_down.shape[0]
    rows, width = block_input.shape
    first_unit = lax.axis_index("mp") * local_units
    unit_index = first_unit + jnp.arange(local_units, dtype=jnp.int32)
    unit_mask = (unit_index < widths[0]).astype(F32)

    x_rows = relative_rows(block_input)
    kinds = []
    for weight in (parent_gate_up[0], parent_gate_up[1], local_gate_up[0], local_gate_up[1]):
        there, here = both_halves(x_rows, weight)
        kinds.append((owner_view(here), owner_view(swap(there, "core", 1))))
    own = []
    for j, order in enumerate(ORDERS):
        own.append(scatter_stream([(k[2 * j : 2 * j + 2], r[2 * j : 2 * j + 2]) for k, r in kinds], order))
    gathered = []
    for pre, order in zip(own, ORDERS):
        pre = pre.astype(BF)
        share = jnp.concatenate([gated(pre[0], pre[1], 1.0)[None], pre[2:]])
        gathered.append(gather_stream(share, order))
    full = []
    for kind in range(3):
        mine = whole_rows(gathered, kind)
        full.append(jnp.concatenate([mine, swap(mine, "core", 1)]))
    parent_hidden, gate_all, up_all = full
    variant_hidden = gated(gate_all, up_all, unit_mask)

    teacher_part = jnp.dot(parent_hidden, parent_down, preferred_element_type=F32).astype(BF)
    student_part = jnp.dot(variant_hidden, local_down, preferred_element_type=F32)
    teacher = teacher_rows(teacher_part.reshape(4, 4, rows // 16, width)).reshape(rows // 4, width)
    split = student_part.reshape(4, rows // 4, width)
    n = width // 2
    loss_scale = 1.0 / math.sqrt(rows)
    sides = []
    for side, (first, second) in enumerate(((1, 3), (3, 1))):
        cut = slice(side * n, side * n + n)
        student = student_quarter(split[:, :, cut], first, second)
        grad = ((student - teacher[:, cut].astype(F32)) * loss_scale).astype(BF)
        sides.append(gather_quarters(grad, second, first))
    output_grad = jnp.concatenate(sides, axis=2).reshape(rows, width)

    half = rows // 2

    def hidden_rows(value):
        return lax.dot_general(value, local_down, (((1,), (1,)), ((), ())), preferred_element_type=F32).astype(BF)

    there = swap(hidden_rows(output_grad[half:]), "core", 1)
    here = hidden_rows(output_grad[:half])
    own_grad = scatter_stream([(owner_view(here), owner_view(there))], "abz").astype(BF)
    mine = gather_stream(own_grad, "abz")[0].reshape(half, local_units)
    hidden_full = jnp.concatenate([mine, swap(mine, "core", 1)])

    grad_down = lax.dot_general(
        variant_hidden, output_grad, (((0,), (0,)), ((), ())), preferred_element_type=F32
    )
    grad_gate_up = gate_up_gradient(x_rows.T, gate_all, up_all, unit_mask, hidden_full)
    return (grad_gate_up[None], grad_down[None])


def solution(mesh):
    axes = ("group", "zl", "y", "core", "mp")
    fine = Mesh(mesh.devices.reshape(4, 2, 4, 2, 4), axes)
    dp = ("zl", "y", "core")
    in_specs = (
        P(None, dp),
        P(None, dp, ("group", "mp")),
        P(("group", "mp"), dp),
        P("group", None, dp, "mp"),
        P("group", "mp", dp),
        P("group"),
    )
    out_specs = (P("group", None, dp, "mp"), P("group", "mp", dp))
    return jax.shard_map(body, mesh=fine, in_specs=in_specs, out_specs=out_specs, check_vma=False)
```

```python
import math

import jax
import jax.numpy as jnp
from jax import lax
from jax.experimental import pallas as pl
from jax.experimental.pallas import tpu as pltpu
from jax.sharding import Mesh
from jax.sharding import PartitionSpec as P

BF, F32 = jnp.bfloat16, jnp.float32
DIMS = {"c": ("core", 1), "a": ("y", 1), "b": ("y", 3), "z": ("zl", 1)}
ORDERS = ("abz", "bza", "zab")


def swap(value, axis, mask):
    size = {"core": 2, "y": 4, "zl": 2, "group": 4, "mp": 4}[axis]
    return lax.ppermute(value, axis, [(i, i ^ mask) for i in range(size)])


def pick(value, axis, index):
    return lax.index_in_dim(value, index, axis, keepdims=False)


def dim_axis(left, dim):
    return 2 + left.index(dim)


def relative_rows(block_input):
    rows, width = block_input.shape

    def kernel(x_ref, o_ref):
        y, z, core = lax.axis_index("y"), lax.axis_index("zl"), lax.axis_index("core")
        owner = ((y ^ (y >> 1)) & 1) * 4 + (y >> 1) * 2 + z
        for block in range(rows // 8):
            half, inner = divmod(block, rows // 16)
            stream, at = divmod(inner, 8)
            o_ref[block] = x_ref[(half ^ core) * (rows // 16) + stream * 8 + (at ^ owner)]

    out = pl.pallas_call(
        kernel,
        out_shape=jax.ShapeDtypeStruct((rows // 8, 8, width), BF),
        in_specs=[pl.BlockSpec(memory_space=pltpu.VMEM)],
        out_specs=pl.BlockSpec(memory_space=pltpu.VMEM),
        cost_estimate=pl.CostEstimate(flops=1000000, bytes_accessed=4 * rows * width, transcendentals=0),
    )(block_input.reshape(rows // 8, 8, width))
    return out.reshape(rows, width)


def owner_view(value):
    return value.reshape(6, 2, 2, 2, value.shape[0] // 48, value.shape[1])


def scatter_stream(kinds, order):
    left = "abz"
    axis = 1 + left.index(order[0])
    send = jnp.stack([(pick(k, axis, 1).astype(F32) + pick(r, axis, 1).astype(F32)).astype(BF) for k, r in kinds])
    keep = jnp.stack([pick(k, axis, 0).astype(F32) + pick(r, axis, 0).astype(F32) for k, r in kinds])
    for step, dim in enumerate(order):
        got = swap(send, *DIMS[dim])
        left = left.replace(dim, "")
        if step == 2:
            return keep + got.astype(F32)
        axis = dim_axis(left, order[step + 1])
        send = pick(keep, axis, 1) + pick(got, axis, 1).astype(F32)
        if step == 0:
            send = send.astype(BF)
        keep = pick(keep, axis, 0) + pick(got, axis, 0).astype(F32)


def gather_stream(value, order):
    left = ""
    for dim in reversed(order):
        got = swap(value, *DIMS[dim])
        left = "".join(sorted(left + dim))
        value = jnp.stack([value, got], axis=dim_axis(left, dim))
    return value


def gated(gate_value, up_value, unit_mask):
    gate_value, up_value = gate_value.astype(F32), up_value.astype(F32)
    return (gate_value * jax.nn.sigmoid(gate_value) * up_value * unit_mask).astype(BF)


def pre_gradient(gate_value, up_value, unit_mask, hidden_grad):
    gate_value, up_value = gate_value.astype(F32), up_value.astype(F32)
    s = jax.nn.sigmoid(gate_value)
    masked = hidden_grad.astype(F32) * unit_mask
    grad_gate = masked * up_value * s * (1.0 + gate_value * (1.0 - s))
    grad_up = masked * gate_value * s
    return grad_gate.astype(BF), grad_up.astype(BF)


def both_halves(x_rows, weight):
    half = x_rows.shape[0] // 2
    there = jnp.dot(x_rows[half:], weight, preferred_element_type=F32).astype(BF)
    here = jnp.dot(x_rows[:half], weight, preferred_element_type=F32)
    return there, here


def whole_rows(streams, kind):
    parts = [s[kind] for s in streams]
    value = jnp.concatenate(parts, axis=0)
    return value.reshape(-1, value.shape[-1])


def sum_over_groups(part, first, second):
    for mask in (first, second):
        part = part + swap(part.astype(BF), "group", mask).astype(F32)
    return part


def ordered(relative, index):
    stacked = jnp.stack(relative)
    return jnp.stack([lax.dynamic_index_in_dim(stacked, index ^ i, 0, keepdims=False) for i in range(4)])


def sum_over_mp(part, first, second, finish):
    m = lax.axis_index("mp")

    def quarter(i):
        return lax.dynamic_index_in_dim(part, i, 0, keepdims=False)

    def pair(one, other):
        return jnp.stack([quarter(m ^ one), quarter(m ^ other)])

    got = swap(pair(first, first ^ second).astype(BF), "mp", first).astype(F32)
    keep = pair(0, second) + got
    got = swap(keep.astype(BF), "mp", second).astype(F32)
    own = finish(keep + got[::-1])
    far = swap(own, "mp", first)
    relative = [None] * 4
    relative[0], relative[second], relative[first], relative[first ^ second] = own[0], own[1], far[0], far[1]
    return ordered(relative, m)


def sum_over_dp(here, there):
    half, n = here.shape
    view = (here.astype(F32) + there.astype(F32)).reshape(2, 3, 2, 2, 2, half // 48, n)
    parts = []
    for stream, order in enumerate(("ab", "ba")):
        left, part = "ab", view[stream]
        for dim in order:
            axis = 1 + left.index(dim)
            part = pick(part, axis, 0) + swap(pick(part, axis, 1).astype(BF), *DIMS[dim]).astype(F32)
            left = left.replace(dim, "")
        parts.append(part)
    both = jnp.stack(parts)
    both = (both + swap(both.astype(BF), *DIMS["z"])[:, :, ::-1].astype(F32)).astype(BF)
    whole = []
    for stream, order in enumerate(("ba", "ab")):
        left, part = "", both[stream]
        for dim in order:
            left = "".join(sorted(left + dim))
            part = jnp.stack([part, swap(part, *DIMS[dim])], axis=1 + left.index(dim))
        whole.append(part)
    return jnp.stack(whole).reshape(half, n)


def body(block_input, parent_gate_up, parent_down, variant_gate_up, variant_down, widths):
    local_gate_up = variant_gate_up[0]
    local_down = variant_down[0]
    local_units = local_down.shape[0]
    rows, width = block_input.shape
    first_unit = lax.axis_index("mp") * local_units
    unit_index = first_unit + jnp.arange(local_units, dtype=jnp.int32)
    unit_mask = (unit_index < widths[0]).astype(F32)

    x_rows = relative_rows(block_input)
    kinds = []
    for weight in (parent_gate_up[0], parent_gate_up[1], local_gate_up[0], local_gate_up[1]):
        there, here = both_halves(x_rows, weight)
        kinds.append((owner_view(here), owner_view(swap(there, "core", 1))))
    own = []
    for j, order in enumerate(ORDERS):
        own.append(scatter_stream([(k[2 * j : 2 * j + 2], r[2 * j : 2 * j + 2]) for k, r in kinds], order))
    def all_rows(shares):
        streams = [gather_stream(share, order) for share, order in zip(shares, ORDERS)]
        full = []
        for kind in range(shares[0].shape[0]):
            mine = whole_rows(streams, kind)
            full.append(jnp.concatenate([mine, swap(mine, "core", 1)]))
        return full

    own = [pre.astype(BF) for pre in own]
    (parent_hidden,) = all_rows([gated(pre[0], pre[1], 1.0)[None] for pre in own])
    teacher_part = jnp.dot(parent_hidden, parent_down, preferred_element_type=F32)
    n = width // 2
    teacher = [sum_over_groups(teacher_part[:, :n], 1, 3), sum_over_groups(teacher_part[:, n:], 3, 1)]
    gate_all, up_all = all_rows([pre[2:] for pre in own])
    variant_hidden = gated(gate_all, up_all, unit_mask)
    student_part = jnp.dot(variant_hidden, local_down, preferred_element_type=F32)
    loss_scale = 1.0 / math.sqrt(rows)

    def finish(total):
        return (total * loss_scale).astype(BF)

    sides = []
    for side, (first, second) in enumerate(((1, 3), (3, 1))):
        part = student_part[:, side * n : side * n + n] - teacher[side]
        sides.append(sum_over_mp(part.reshape(4, rows // 4, n), first, second, finish))
    output_grad = jnp.concatenate(sides, axis=2).reshape(rows, width)

    half = rows // 2

    def hidden_rows(value):
        return lax.dot_general(value, local_down, (((1,), (1,)), ((), ())), preferred_element_type=F32)

    there = swap(hidden_rows(output_grad[half:]).astype(BF), "core", 1)
    here = hidden_rows(output_grad[:half])
    mine = sum_over_dp(here, there)
    hidden_full = jnp.concatenate([mine, swap(mine, "core", 1)])

    grad_down = lax.dot_general(
        variant_hidden, output_grad, (((0,), (0,)), ((), ())), preferred_element_type=F32
    )
    pre_grads = pre_gradient(gate_all, up_all, unit_mask, hidden_full)
    grad_gate_up = jnp.stack(
        [lax.dot_general(x_rows, g, (((0,), (0,)), ((), ())), preferred_element_type=F32) for g in pre_grads]
    )
    return (grad_gate_up[None], grad_down[None])


def solution(mesh):
    axes = ("group", "zl", "y", "core", "mp")
    fine = Mesh(mesh.devices.reshape(4, 2, 4, 2, 4), axes)
    dp = ("zl", "y", "core")
    in_specs = (
        P(None, dp),
        P(None, dp, ("group", "mp")),
        P(("group", "mp"), dp),
        P("group", None, dp, "mp"),
        P("group", "mp", dp),
        P("group"),
    )
    out_specs = (P("group", None, dp, "mp"), P("group", "mp", dp))
    return jax.shard_map(body, mesh=fine, in_specs=in_specs, out_specs=out_specs, check_vma=False)
```

```python
import math

import jax
import jax.numpy as jnp
from jax import lax
from jax.experimental import pallas as pl
from jax.experimental.pallas import tpu as pltpu
from jax.sharding import Mesh
from jax.sharding import PartitionSpec as P

BF, F32 = jnp.bfloat16, jnp.float32
DIMS = {"c": ("core", 1), "a": ("y", 1), "b": ("y", 3), "z": ("zl", 1)}
ORDERS = ("abz", "bza", "zab")


def swap(value, axis, mask):
    size = {"core": 2, "y": 4, "zl": 2, "group": 4, "mp": 4}[axis]
    return lax.ppermute(value, axis, [(i, i ^ mask) for i in range(size)])


def pick(value, axis, index):
    return lax.index_in_dim(value, index, axis, keepdims=False)


def dim_axis(left, dim):
    return 2 + left.index(dim)


def relative_rows(block_input):
    rows, width = block_input.shape

    def kernel(x_ref, o_ref):
        y, z, core = lax.axis_index("y"), lax.axis_index("zl"), lax.axis_index("core")
        owner = ((y ^ (y >> 1)) & 1) * 4 + (y >> 1) * 2 + z
        for block in range(rows // 8):
            half, inner = divmod(block, rows // 16)
            stream, at = divmod(inner, 8)
            o_ref[block] = x_ref[(half ^ core) * (rows // 16) + stream * 8 + (at ^ owner)]

    out = pl.pallas_call(
        kernel,
        out_shape=jax.ShapeDtypeStruct((rows // 8, 8, width), BF),
        in_specs=[pl.BlockSpec(memory_space=pltpu.VMEM)],
        out_specs=pl.BlockSpec(memory_space=pltpu.VMEM),
        cost_estimate=pl.CostEstimate(flops=1000000, bytes_accessed=4 * rows * width, transcendentals=0),
    )(block_input.reshape(rows // 8, 8, width))
    return out.reshape(rows, width)


def owner_view(value):
    return value.reshape(value.shape[0], 6, 2, 2, 2, value.shape[1] // 48, value.shape[2])


def scatter_stream(pairs, order):
    left = "abz"
    axis = dim_axis(left, order[0])

    def part(index):
        return jnp.concatenate([pick(k, axis, index).astype(F32) + pick(r, axis, index).astype(F32) for k, r in pairs])

    send, keep = part(1).astype(BF), part(0)
    for step, dim in enumerate(order):
        got = swap(send, *DIMS[dim])
        left = left.replace(dim, "")
        if step == 2:
            return keep + got.astype(F32)
        axis = dim_axis(left, order[step + 1])
        send = pick(keep, axis, 1) + pick(got, axis, 1).astype(F32)
        if step == 0:
            send = send.astype(BF)
        keep = pick(keep, axis, 0) + pick(got, axis, 0).astype(F32)


def gather_y(parts):
    parts, lefts = list(parts), ["", ""]
    for dims in ("ba", "ab"):
        for i, dim in enumerate(dims):
            lefts[i] = "".join(sorted(lefts[i] + dim))
            parts[i] = jnp.stack([parts[i], swap(parts[i], *DIMS[dim])], axis=dim_axis(lefts[i], dim))
    value = jnp.concatenate(parts, axis=1)
    return value.reshape(value.shape[0], -1, value.shape[-1])


def gather_z(own):
    return jnp.stack([own, swap(own, *DIMS["z"])], axis=2)


def with_other_core(mine):
    return jnp.concatenate([mine, swap(mine, "core", 1)], axis=1)


def gated(gate_value, up_value, unit_mask):
    gate_value, up_value = gate_value.astype(F32), up_value.astype(F32)
    return (gate_value * jax.nn.sigmoid(gate_value) * up_value * unit_mask).astype(BF)


def pre_gradient(gate_value, up_value, unit_mask, hidden_grad):
    gate_value, up_value = gate_value.astype(F32), up_value.astype(F32)
    s = jax.nn.sigmoid(gate_value)
    masked = hidden_grad.astype(F32) * unit_mask
    grad_gate = masked * up_value * s * (1.0 + gate_value * (1.0 - s))
    grad_up = masked * gate_value * s
    return grad_gate.astype(BF), grad_up.astype(BF)


def both_halves(x_rows, weight):
    half = x_rows.shape[0] // 2
    there = jnp.einsum("td,kdf->ktf", x_rows[half:], weight, preferred_element_type=F32).astype(BF)
    here = jnp.einsum("td,kdf->ktf", x_rows[:half], weight, preferred_element_type=F32)
    return there, here


def add_group(part, mask):
    return part + swap(part.astype(BF), "group", mask).astype(F32)


def ordered(relative, index):
    stacked = jnp.stack(relative)
    return jnp.stack([lax.dynamic_index_in_dim(stacked, index ^ i, 0, keepdims=False) for i in range(4)])


def sum_over_mp(part, first, second, finish):
    m = lax.axis_index("mp")

    def quarter(i):
        return lax.dynamic_index_in_dim(part, i, 0, keepdims=False)

    def pair(one, other):
        return jnp.stack([quarter(m ^ one), quarter(m ^ other)])

    got = swap(pair(first, first ^ second).astype(BF), "mp", first).astype(F32)
    keep = pair(0, second) + got
    got = swap(keep.astype(BF), "mp", second).astype(F32)
    own = finish(keep + got[::-1])
    far = swap(own, "mp", first)
    relative = [None] * 4
    relative[0], relative[second], relative[first], relative[first ^ second] = own[0], own[1], far[0], far[1]
    return ordered(relative, m)


def sum_over_dp(here, there):
    half, n = here.shape
    view = (here.astype(F32) + there.astype(F32)).reshape(2, 3, 2, 2, 2, half // 48, n)
    parts = []
    for stream, order in enumerate(("ab", "ba")):
        left, part = "ab", view[stream]
        for dim in order:
            axis = 1 + left.index(dim)
            part = pick(part, axis, 0) + swap(pick(part, axis, 1).astype(BF), *DIMS[dim]).astype(F32)
            left = left.replace(dim, "")
        parts.append(part)
    both = jnp.stack(parts)
    return both + swap(both.astype(BF), *DIMS["z"])[:, :, ::-1].astype(F32)


def body(block_input, parent_gate_up, parent_down, variant_gate_up, variant_down, widths):
    local_gate_up = variant_gate_up[0]
    local_down = variant_down[0]
    local_units = local_down.shape[0]
    rows, width = block_input.shape
    first_unit = lax.axis_index("mp") * local_units
    unit_index = first_unit + jnp.arange(local_units, dtype=jnp.int32)
    unit_mask = (unit_index < widths[0]).astype(F32)

    x_rows = relative_rows(block_input)
    pairs = []
    for weight in (parent_gate_up, local_gate_up):
        there, here = both_halves(x_rows, weight)
        pairs.append((owner_view(here), owner_view(swap(there, "core", 1))))
    own = []
    for j, order in enumerate(ORDERS):
        cut = slice(2 * j, 2 * j + 2)
        own.append(scatter_stream([(k[:, cut], r[:, cut]) for k, r in pairs], order))
    own = jnp.concatenate(own, axis=1).astype(BF)

    hidden_both = gather_z(gated(own[0], own[1], 1.0)[None])
    pre_own, hidden_both = lax.optimization_barrier((own[2:], hidden_both))
    parent_hidden = with_other_core(gather_y((hidden_both[:, :3], hidden_both[:, 3:])))[0]
    teacher_part = jnp.dot(parent_hidden, parent_down, preferred_element_type=F32)
    n = width // 2
    teacher = [add_group(teacher_part[:, :n], 1), add_group(teacher_part[:, n:], 3)]

    pre_both = gather_z(pre_own)
    pre_mine = gather_y((pre_both[:, :3], pre_both[:, 3:]))
    pre_mine, teacher = lax.optimization_barrier((pre_mine, teacher))
    teacher = [add_group(teacher[0], 3), add_group(teacher[1], 1)]
    gate_all, up_all = with_other_core(pre_mine)
    variant_hidden = gated(gate_all, up_all, unit_mask)
    student_part = jnp.dot(variant_hidden, local_down, preferred_element_type=F32)
    loss_scale = 1.0 / math.sqrt(rows)

    def finish(total):
        return (total * loss_scale).astype(BF)

    sides = []
    for side, (first, second) in enumerate(((1, 3), (3, 1))):
        part = student_part[:, side * n : side * n + n] - teacher[side]
        sides.append(sum_over_mp(part.reshape(4, rows // 4, n), first, second, finish))
    output_grad = jnp.concatenate(sides, axis=2).reshape(rows, width)

    half = rows // 2

    def hidden_rows(value):
        return lax.dot_general(value, local_down, (((1,), (1,)), ((), ())), preferred_element_type=F32)

    there = swap(hidden_rows(output_grad[half:]).astype(BF), "core", 1)
    here = hidden_rows(output_grad[:half])
    grad_down = lax.dot_general(
        variant_hidden, output_grad, (((0,), (0,)), ((), ())), preferred_element_type=F32
    )
    summed = sum_over_dp(here, there)
    summed, grad_down, x_t = lax.optimization_barrier((summed, grad_down, x_rows.T))
    summed = summed.astype(BF)[:, None]
    hidden_full = with_other_core(gather_y((summed[0], summed[1])))[0]
    pre_grads = lax.optimization_barrier(pre_gradient(gate_all, up_all, unit_mask, hidden_full))
    grad_gate_up = jnp.stack([jnp.dot(x_t, g, preferred_element_type=F32) for g in pre_grads])
    return (grad_gate_up[None], grad_down[None])


def solution(mesh):
    axes = ("group", "zl", "y", "core", "mp")
    fine = Mesh(mesh.devices.reshape(4, 2, 4, 2, 4), axes)
    dp = ("zl", "y", "core")
    in_specs = (
        P(None, dp),
        P(None, dp, ("group", "mp")),
        P(("group", "mp"), dp),
        P("group", None, dp, "mp"),
        P("group", "mp", dp),
        P("group"),
    )
    out_specs = (P("group", None, dp, "mp"), P("group", "mp", dp))
    return jax.shard_map(body, mesh=fine, in_specs=in_specs, out_specs=out_specs, check_vma=False)
```

```python
import math

import jax
import jax.numpy as jnp
from jax import lax
from jax.experimental import pallas as pl
from jax.experimental.pallas import tpu as pltpu
from jax.sharding import Mesh
from jax.sharding import PartitionSpec as P

BF, F32 = jnp.bfloat16, jnp.float32
DIMS = {"c": ("core", 1), "a": ("y", 1), "b": ("y", 3), "z": ("zl", 1)}
ORDERS = ("abz", "bza", "zab")


def swap(value, axis, mask):
    size = {"core": 2, "y": 4, "zl": 2, "group": 4, "mp": 4}[axis]
    return lax.ppermute(value, axis, [(i, i ^ mask) for i in range(size)])


def pick(value, axis, index):
    return lax.index_in_dim(value, index, axis, keepdims=False)


def dim_axis(left, dim):
    return 2 + left.index(dim)


def relative_rows(block_input):
    rows, width = block_input.shape

    def kernel(x_ref, o_ref):
        y, z, core = lax.axis_index("y"), lax.axis_index("zl"), lax.axis_index("core")
        owner = ((y ^ (y >> 1)) & 1) * 4 + (y >> 1) * 2 + z
        for block in range(rows // 8):
            half, inner = divmod(block, rows // 16)
            stream, at = divmod(inner, 8)
            o_ref[block] = x_ref[(half ^ core) * (rows // 16) + stream * 8 + (at ^ owner)]

    out = pl.pallas_call(
        kernel,
        out_shape=jax.ShapeDtypeStruct((rows // 8, 8, width), BF),
        in_specs=[pl.BlockSpec(memory_space=pltpu.VMEM)],
        out_specs=pl.BlockSpec(memory_space=pltpu.VMEM),
        cost_estimate=pl.CostEstimate(flops=1000000, bytes_accessed=4 * rows * width, transcendentals=0),
    )(block_input.reshape(rows // 8, 8, width))
    return out.reshape(rows, width)


def owner_view(value):
    return value.reshape(1, 6, 2, 2, 2, value.shape[0] // 48, value.shape[1])


def scatter_stream(pairs, order):
    left = "abz"
    axis = dim_axis(left, order[0])

    def part(index):
        return jnp.concatenate([pick(k, axis, index).astype(F32) + pick(r, axis, index).astype(F32) for k, r in pairs])

    send, keep = part(1).astype(BF), part(0)
    for step, dim in enumerate(order):
        got = swap(send, *DIMS[dim])
        left = left.replace(dim, "")
        if step == 2:
            return keep + got.astype(F32)
        axis = dim_axis(left, order[step + 1])
        send = pick(keep, axis, 1) + pick(got, axis, 1).astype(F32)
        if step == 0:
            send = send.astype(BF)
        keep = pick(keep, axis, 0) + pick(got, axis, 0).astype(F32)


def gather_y(parts):
    parts, lefts = list(parts), ["", ""]
    for dims in ("ba", "ab"):
        for i, dim in enumerate(dims):
            lefts[i] = "".join(sorted(lefts[i] + dim))
            parts[i] = jnp.stack([parts[i], swap(parts[i], *DIMS[dim])], axis=dim_axis(lefts[i], dim))
    value = jnp.concatenate(parts, axis=1)
    return value.reshape(value.shape[0], -1, value.shape[-1])


def gather_z(own):
    return jnp.stack([own, swap(own, *DIMS["z"])], axis=2)


def with_other_core(mine):
    return jnp.concatenate([mine, swap(mine, "core", 1)], axis=1)


def gated(gate_value, up_value, unit_mask):
    gate_value, up_value = gate_value.astype(F32), up_value.astype(F32)
    return (gate_value * jax.nn.sigmoid(gate_value) * up_value * unit_mask).astype(BF)


def pre_gradient(gate_value, up_value, unit_mask, hidden_grad):
    gate_value, up_value = gate_value.astype(F32), up_value.astype(F32)
    s = jax.nn.sigmoid(gate_value)
    masked = hidden_grad.astype(F32) * unit_mask
    grad_gate = masked * up_value * s * (1.0 + gate_value * (1.0 - s))
    grad_up = masked * gate_value * s
    return grad_gate.astype(BF), grad_up.astype(BF)


def both_halves(x_rows, weight):
    half = x_rows.shape[0] // 2
    there = jnp.dot(x_rows[half:], weight, preferred_element_type=F32).astype(BF)
    here = jnp.dot(x_rows[:half], weight, preferred_element_type=F32)
    return there, here


def add_group(part, mask):
    return part + swap(part.astype(BF), "group", mask).astype(F32)


def ordered(relative, index):
    stacked = jnp.stack(relative)
    return jnp.stack([lax.dynamic_index_in_dim(stacked, index ^ i, 0, keepdims=False) for i in range(4)])


def sum_over_mp(part, first, second, finish):
    m = lax.axis_index("mp")

    def quarter(i):
        return lax.dynamic_index_in_dim(part, i, 0, keepdims=False)

    def pair(one, other):
        return jnp.stack([quarter(m ^ one), quarter(m ^ other)])

    got = swap(pair(first, first ^ second).astype(BF), "mp", first).astype(F32)
    keep = pair(0, second) + got
    got = swap(keep.astype(BF), "mp", second).astype(F32)
    own = finish(keep + got[::-1])
    far = swap(own, "mp", first)
    relative = [None] * 4
    relative[0], relative[second], relative[first], relative[first ^ second] = own[0], own[1], far[0], far[1]
    return ordered(relative, m)


def sum_over_dp(here, there):
    half, n = here.shape
    view = (here.astype(F32) + there.astype(F32)).reshape(2, 3, 2, 2, 2, half // 48, n)
    parts = []
    for stream, order in enumerate(("ab", "ba")):
        left, part = "ab", view[stream]
        for dim in order:
            axis = 1 + left.index(dim)
            part = pick(part, axis, 0) + swap(pick(part, axis, 1).astype(BF), *DIMS[dim]).astype(F32)
            left = left.replace(dim, "")
        parts.append(part)
    both = jnp.stack(parts)
    return both + swap(both.astype(BF), *DIMS["z"])[:, :, ::-1].astype(F32)


def body(block_input, parent_gate_up, parent_down, variant_gate_up, variant_down, widths):
    local_gate_up = variant_gate_up[0]
    local_down = variant_down[0]
    local_units = local_down.shape[0]
    rows, width = block_input.shape
    first_unit = lax.axis_index("mp") * local_units
    unit_index = first_unit + jnp.arange(local_units, dtype=jnp.int32)
    unit_mask = (unit_index < widths[0]).astype(F32)

    x_rows = relative_rows(block_input)
    pairs = []
    for weight in (parent_gate_up[0], parent_gate_up[1], local_gate_up[0], local_gate_up[1]):
        there, here = both_halves(x_rows, weight)
        pairs.append((owner_view(here), owner_view(swap(there, "core", 1))))
    own = []
    for j, order in enumerate(ORDERS):
        cut = slice(2 * j, 2 * j + 2)
        own.append(scatter_stream([(k[:, cut], r[:, cut]) for k, r in pairs], order))
    own = jnp.concatenate(own, axis=1).astype(BF)

    hidden_both = gather_z(gated(own[0], own[1], 1.0)[None])
    pre_own, hidden_both = lax.optimization_barrier((own[2:], hidden_both))
    parent_hidden = with_other_core(gather_y((hidden_both[:, :3], hidden_both[:, 3:])))[0]
    teacher_part = jnp.dot(parent_hidden, parent_down, preferred_element_type=F32)
    n = width // 2
    pre_both = gather_z(pre_own)
    first_sends = (teacher_part[:, :n].astype(BF), teacher_part[:, n:].astype(BF))
    pre_both, first_sends = lax.optimization_barrier((pre_both, first_sends))
    teacher = [
        part + swap(send, "group", mask).astype(F32)
        for part, send, mask in zip((teacher_part[:, :n], teacher_part[:, n:]), first_sends, (1, 3))
    ]
    pre_mine = gather_y((pre_both[:, :3], pre_both[:, 3:]))
    pre_mine, teacher = lax.optimization_barrier((pre_mine, teacher))
    teacher = [add_group(teacher[0], 3), add_group(teacher[1], 1)]
    gate_all, up_all = with_other_core(pre_mine)
    variant_hidden = gated(gate_all, up_all, unit_mask)
    student_part = jnp.dot(variant_hidden, local_down, preferred_element_type=F32)
    loss_scale = 1.0 / math.sqrt(rows)

    def finish(total):
        return (total * loss_scale).astype(BF)

    sides = []
    for side, (first, second) in enumerate(((1, 3), (3, 1))):
        part = student_part[:, side * n : side * n + n] - teacher[side]
        sides.append(sum_over_mp(part.reshape(4, rows // 4, n), first, second, finish))
    output_grad = jnp.concatenate(sides, axis=2).reshape(rows, width)

    half = rows // 2

    def hidden_rows(value):
        return lax.dot_general(value, local_down, (((1,), (1,)), ((), ())), preferred_element_type=F32)

    there = swap(hidden_rows(output_grad[half:]).astype(BF), "core", 1)
    here = hidden_rows(output_grad[:half])
    grad_down = lax.dot_general(
        variant_hidden, output_grad, (((0,), (0,)), ((), ())), preferred_element_type=F32
    )
    summed = sum_over_dp(here, there)
    summed, grad_down, x_t = lax.optimization_barrier((summed, grad_down, x_rows.T))
    summed = summed.astype(BF)[:, None]
    hidden_full = with_other_core(gather_y((summed[0], summed[1])))[0]
    pre_grads = lax.optimization_barrier(pre_gradient(gate_all, up_all, unit_mask, hidden_full))
    grad_gate_up = jnp.stack([jnp.dot(x_t, g, preferred_element_type=F32) for g in pre_grads])
    return (grad_gate_up[None], grad_down[None])


def solution(mesh):
    axes = ("group", "zl", "y", "core", "mp")
    fine = Mesh(mesh.devices.reshape(4, 2, 4, 2, 4), axes)
    dp = ("zl", "y", "core")
    in_specs = (
        P(None, dp),
        P(None, dp, ("group", "mp")),
        P(("group", "mp"), dp),
        P("group", None, dp, "mp"),
        P("group", "mp", dp),
        P("group"),
    )
    out_specs = (P("group", None, dp, "mp"), P("group", "mp", dp))
    return jax.shard_map(body, mesh=fine, in_specs=in_specs, out_specs=out_specs, check_vma=False)
```

```python
import math

import jax
import jax.numpy as jnp
from jax import lax
from jax.experimental import pallas as pl
from jax.experimental.pallas import tpu as pltpu
from jax.sharding import Mesh
from jax.sharding import PartitionSpec as P

BF, F32 = jnp.bfloat16, jnp.float32
DIMS = {"c": ("core", 1), "a": ("y", 1), "b": ("y", 3), "z": ("zl", 1)}
ORDERS = ("abz", "bza", "zab")


def swap(value, axis, mask):
    size = {"core": 2, "y": 4, "zl": 2, "group": 4, "mp": 4}[axis]
    return lax.ppermute(value, axis, [(i, i ^ mask) for i in range(size)])


def pick(value, axis, index):
    return lax.index_in_dim(value, index, axis, keepdims=False)


def dim_axis(left, dim):
    return 2 + left.index(dim)


def relative_rows(block_input):
    rows, width = block_input.shape

    def kernel(x_ref, o_ref):
        y, z, core = lax.axis_index("y"), lax.axis_index("zl"), lax.axis_index("core")
        owner = ((y ^ (y >> 1)) & 1) * 4 + (y >> 1) * 2 + z
        for block in range(rows // 8):
            half, inner = divmod(block, rows // 16)
            stream, at = divmod(inner, 8)
            o_ref[block] = x_ref[(half ^ core) * (rows // 16) + stream * 8 + (at ^ owner)]

    out = pl.pallas_call(
        kernel,
        out_shape=jax.ShapeDtypeStruct((rows // 8, 8, width), BF),
        in_specs=[pl.BlockSpec(memory_space=pltpu.VMEM)],
        out_specs=pl.BlockSpec(memory_space=pltpu.VMEM),
        cost_estimate=pl.CostEstimate(flops=1000000, bytes_accessed=4 * rows * width, transcendentals=0),
    )(block_input.reshape(rows // 8, 8, width))
    return out.reshape(rows, width)


def owner_view(value):
    return value.reshape(6, 2, 2, 2, value.shape[0] // 48, value.shape[1])


def scatter_stream(kinds, order):
    left = "abz"
    axis = 1 + left.index(order[0])
    send = jnp.stack([(pick(k, axis, 1).astype(F32) + pick(r, axis, 1).astype(F32)).astype(BF) for k, r in kinds])
    keep = jnp.stack([pick(k, axis, 0).astype(F32) + pick(r, axis, 0).astype(F32) for k, r in kinds])
    for step, dim in enumerate(order):
        got = swap(send, *DIMS[dim])
        left = left.replace(dim, "")
        if step == 2:
            return keep + got.astype(F32)
        axis = dim_axis(left, order[step + 1])
        send = pick(keep, axis, 1) + pick(got, axis, 1).astype(F32)
        if step == 0:
            send = send.astype(BF)
        keep = pick(keep, axis, 0) + pick(got, axis, 0).astype(F32)


def gather_stream(value, order):
    left = ""
    for dim in reversed(order):
        got = swap(value, *DIMS[dim])
        left = "".join(sorted(left + dim))
        value = jnp.stack([value, got], axis=dim_axis(left, dim))
    return value


def gated(gate_value, up_value, unit_mask):
    gate_value, up_value = gate_value.astype(F32), up_value.astype(F32)
    return (gate_value * jax.nn.sigmoid(gate_value) * up_value * unit_mask).astype(BF)


def pre_gradient(gate_value, up_value, unit_mask, hidden_grad):
    gate_value, up_value = gate_value.astype(F32), up_value.astype(F32)
    s = jax.nn.sigmoid(gate_value)
    masked = hidden_grad.astype(F32) * unit_mask
    grad_gate = masked * up_value * s * (1.0 + gate_value * (1.0 - s))
    grad_up = masked * gate_value * s
    return grad_gate.astype(BF), grad_up.astype(BF)


def both_halves(x_rows, weight):
    half = x_rows.shape[0] // 2
    there = jnp.dot(x_rows[half:], weight, preferred_element_type=F32).astype(BF)
    here = jnp.dot(x_rows[:half], weight, preferred_element_type=F32)
    return there, here


def whole_rows(streams, kind):
    parts = [s[kind] for s in streams]
    value = jnp.concatenate(parts, axis=0)
    return value.reshape(-1, value.shape[-1])


def sum_over_groups(part, first, second):
    for mask in (first, second):
        part = part + swap(part.astype(BF), "group", mask).astype(F32)
    return part


def ordered(relative, index):
    stacked = jnp.stack(relative)
    return jnp.stack([lax.dynamic_index_in_dim(stacked, index ^ i, 0, keepdims=False) for i in range(4)])


def sum_over_mp(part, first, second, finish):
    m = lax.axis_index("mp")

    def quarter(i):
        return lax.dynamic_index_in_dim(part, i, 0, keepdims=False)

    def pair(one, other):
        return jnp.stack([quarter(m ^ one), quarter(m ^ other)])

    got = swap(pair(first, first ^ second).astype(BF), "mp", first).astype(F32)
    keep = pair(0, second) + got
    got = swap(keep.astype(BF), "mp", second).astype(F32)
    own = finish(keep + got[::-1])
    far = swap(own, "mp", first)
    relative = [None] * 4
    relative[0], relative[second], relative[first], relative[first ^ second] = own[0], own[1], far[0], far[1]
    return ordered(relative, m)


def gather_y(parts):
    parts, lefts = list(parts), ["", ""]
    for dims in ("ba", "ab"):
        for i, dim in enumerate(dims):
            lefts[i] = "".join(sorted(lefts[i] + dim))
            parts[i] = jnp.stack([parts[i], swap(parts[i], *DIMS[dim])], axis=dim_axis(lefts[i], dim))
    value = jnp.concatenate(parts, axis=1)
    return value.reshape(value.shape[0], -1, value.shape[-1])


def sum_over_dp(here, there):
    half, n = here.shape
    view = (here.astype(F32) + there.astype(F32)).reshape(2, 3, 2, 2, 2, half // 48, n)
    parts = []
    for stream, order in enumerate(("ab", "ba")):
        left, part = "ab", view[stream]
        for dim in order:
            axis = 1 + left.index(dim)
            part = pick(part, axis, 0) + swap(pick(part, axis, 1).astype(BF), *DIMS[dim]).astype(F32)
            left = left.replace(dim, "")
        parts.append(part)
    both = jnp.stack(parts)
    return both + swap(both.astype(BF), *DIMS["z"])[:, :, ::-1].astype(F32)


def body(block_input, parent_gate_up, parent_down, variant_gate_up, variant_down, widths):
    local_gate_up = variant_gate_up[0]
    local_down = variant_down[0]
    local_units = local_down.shape[0]
    rows, width = block_input.shape
    first_unit = lax.axis_index("mp") * local_units
    unit_index = first_unit + jnp.arange(local_units, dtype=jnp.int32)
    unit_mask = (unit_index < widths[0]).astype(F32)

    x_rows = relative_rows(block_input)
    kinds = []
    for weight in (parent_gate_up[0], parent_gate_up[1], local_gate_up[0], local_gate_up[1]):
        there, here = both_halves(x_rows, weight)
        kinds.append((owner_view(here), owner_view(swap(there, "core", 1))))
    own = []
    for j, order in enumerate(ORDERS):
        own.append(scatter_stream([(k[2 * j : 2 * j + 2], r[2 * j : 2 * j + 2]) for k, r in kinds], order))
    def all_rows(shares):
        streams = [gather_stream(share, order) for share, order in zip(shares, ORDERS)]
        full = []
        for kind in range(shares[0].shape[0]):
            mine = whole_rows(streams, kind)
            full.append(jnp.concatenate([mine, swap(mine, "core", 1)]))
        return full

    own = [pre.astype(BF) for pre in own]
    (parent_hidden,) = all_rows([gated(pre[0], pre[1], 1.0)[None] for pre in own])
    teacher_part = jnp.dot(parent_hidden, parent_down, preferred_element_type=F32)
    n = width // 2
    teacher = [sum_over_groups(teacher_part[:, :n], 1, 3), sum_over_groups(teacher_part[:, n:], 3, 1)]
    gate_all, up_all = all_rows([pre[2:] for pre in own])
    variant_hidden = gated(gate_all, up_all, unit_mask)
    student_part = jnp.dot(variant_hidden, local_down, preferred_element_type=F32)
    loss_scale = 1.0 / math.sqrt(rows)

    def finish(total):
        return (total * loss_scale).astype(BF)

    sides = []
    for side, (first, second) in enumerate(((1, 3), (3, 1))):
        part = student_part[:, side * n : side * n + n] - teacher[side]
        sides.append(sum_over_mp(part.reshape(4, rows // 4, n), first, second, finish))
    output_grad = jnp.concatenate(sides, axis=2).reshape(rows, width)

    half = rows // 2

    def hidden_rows(value):
        return lax.dot_general(value, local_down, (((1,), (1,)), ((), ())), preferred_element_type=F32)

    there = swap(hidden_rows(output_grad[half:]).astype(BF), "core", 1)
    here = hidden_rows(output_grad[:half])
    grad_down = lax.dot_general(
        variant_hidden, output_grad, (((0,), (0,)), ((), ())), preferred_element_type=F32
    )
    summed = sum_over_dp(here, there)
    summed, grad_down, x_t = lax.optimization_barrier((summed, grad_down, x_rows.T))
    summed = summed.astype(BF)[:, None]
    mine = gather_y((summed[0], summed[1]))[0]
    hidden_full = jnp.concatenate([mine, swap(mine, "core", 1)])
    pre_grads = lax.optimization_barrier(pre_gradient(gate_all, up_all, unit_mask, hidden_full))
    grad_gate_up = jnp.stack([jnp.dot(x_t, g, preferred_element_type=F32) for g in pre_grads])
    return (grad_gate_up[None], grad_down[None])


def solution(mesh):
    axes = ("group", "zl", "y", "core", "mp")
    fine = Mesh(mesh.devices.reshape(4, 2, 4, 2, 4), axes)
    dp = ("zl", "y", "core")
    in_specs = (
        P(None, dp),
        P(None, dp, ("group", "mp")),
        P(("group", "mp"), dp),
        P("group", None, dp, "mp"),
        P("group", "mp", dp),
        P("group"),
    )
    out_specs = (P("group", None, dp, "mp"), P("group", "mp", dp))
    return jax.shard_map(body, mesh=fine, in_specs=in_specs, out_specs=out_specs, check_vma=False)
```
